32 devices in a mesh: expert: 4 (over z), neuron: 8 (over y, x, core).
Axes of the slice: x: 2, y: 2, z: 4, core: 2. Of those that a mesh axis runs over, the one named last changes fastest.
Arguments:
- tokens: bfloat16 [256, 4096], P('neuron'), may hold values from -6 to 6
- route_logits: float32 [256, 2], replicated, may hold values from -6 to 6
- expert_ids: int32 [256, 2], replicated, may hold values from 0 to 3, all different within a row; in each aligned block of 256 rows (0 to 255, 256 to 511, ...) at most 128 rows name the same one
- block_live: int32 [4, 224], P('expert', 'neuron'), may hold values 0 or 1
- w_gate: bfloat16 [4, 4096, 14336], P('expert', None, 'neuron'), may hold values from -0.09375 to 0.09375
- w_up: bfloat16 [4, 4096, 14336], P('expert', None, 'neuron'), may hold values from -0.09375 to 0.09375
- w_down: bfloat16 [4, 14336, 4096], P('expert', 'neuron'), may hold values from -0.046875 to 0.046875
Outputs:
- mixed: bfloat16 [256, 4096], P('neuron')
The draws below stay inside these ranges and needn't reach their ends.
Inputs may be any that keep to these rules, and one draw needn't show every extreme that they name: `expert_ids`: each token names two different experts; no expert is named by more than 128 tokens, a bound that some block reaches; every expert is named.
All inputs are finite; a program needn't handle non-finite values. No bound on the sum of `block_live` on one device may be relied on, other than what follows from the above.
Results may differ from the reference program's by a relative error of at most 0.0049.
Values may be sent and summed in bfloat16 or wider, within the bound.
A program may use at most 128 MiB of HBM per device.

```python
import math
import jax
import jax.numpy as jnp
import numpy as np
from jax import lax

D = 4096
FF = 14336
TOP = 2
BLK = 64
EXPERTS = 4
TOKENS = 256
CAP = 128


def place_ends(values, rng, low, high):
    place = [jax.random.randint(jax.random.fold_in(rng, axis), (), 0, length) for axis, length in enumerate(values.shape)]
    main_axis = values.shape.index(max(values.shape))
    neighbour = place[:main_axis] + [(place[main_axis] + 1) % values.shape[main_axis]] + place[main_axis + 1:]
    return values.at[tuple(place)].set(low).at[tuple(neighbour)].set(high)


def steps_of(key, shape, pieces, low, high):
    def one(position, blocks):
        draws = jax.random.uniform(jax.random.fold_in(jax.random.fold_in(key, 6), position), (blocks,), jnp.float32, low / len(pieces), high / len(pieces))
        return jnp.repeat(jnp.exp(draws), shape[position] // blocks).reshape((-1,) + (1,) * (len(shape) - position - 1))

    loudness = one(*pieces[0])
    for cut in pieces[1:]:
        loudness = loudness * one(*cut)
    return loudness


def assign_block(key, own, number, rows, count, top, limit, slope):
    ranking = jax.random.permutation(key, count)
    heavy_load, common = shares(count, rows * top, limit, slope, True), shares(count, rows * top, limit, slope, False)
    places = jnp.arange(count)

    def named(lengths, offset_by):
        used = int((lengths > 0).sum())
        fixed = max(1, used // 4)
        moved = fixed + (places - fixed + offset_by * (used - fixed)) % max(1, count - fixed)
        return jnp.zeros((count,), jnp.int32).at[ranking[jnp.where(places < fixed, places, moved)]].set(jnp.asarray(lengths, jnp.int32))

    lengths = jnp.where(number % 4 == 0, named(heavy_load, number // 4), named(common, number - number // 4 - 1))
    mixed = jax.random.permutation(jax.random.fold_in(own, 3), count)
    donor, sink = mixed[0:count // 2 * 2:2], mixed[1:count // 2 * 2:2]
    room = jnp.minimum(lengths[donor] - 1, limit - lengths[sink]) // 2
    room = jnp.where((donor == ranking[0]) | (sink == ranking[0]) | (lengths[sink] == 0), 0, jnp.maximum(room, 0))
    moved = jax.random.randint(jax.random.fold_in(own, 4), (count // 2,), 0, 1 << 20) % (room + 1)
    lengths = lengths.at[donor].add(-moved).at[sink].add(moved)
    items = jnp.searchsorted(jnp.cumsum(lengths), jnp.arange(rows * top), side="right").astype(jnp.int32)
    listing = items.reshape(top, rows).T
    listing = listing[jax.random.permutation(jax.random.fold_in(own, 1), rows)]
    offset_by = jax.random.randint(jax.random.fold_in(own, 2), (rows, 1), 0, top)
    return jnp.take_along_axis(listing, (jnp.arange(top)[None, :] + offset_by) % top, axis=1)


def shares(count, total, bound, slope, full):
    portions = [(1 << 20) // math.isqrt(rank ** slope) + 1 for rank in range(1, count + 1)]
    largest = bound if full else min(bound, max(-(-total // count), total * portions[0] // sum(portions)))
    least = 1 if total - largest >= count - 1 else 0
    holding, spare = [largest] + [least] * (count - 1), total - largest - least * (count - 1)
    while spare > 0:
        candidates = [i for i in range(1, count) if holding[i] < largest] or [i for i in range(1, count) if holding[i] < bound]
        pool, budget = sum([portions[i] for i in candidates]), spare
        for i in candidates:
            extra = min(bound - holding[i], max(1, budget * portions[i] // pool), spare)
            holding[i] = holding[i] + extra
            spare = spare - extra
    return np.array(holding)


def bell_draw(stream_key, dims, deviation, most, cuts=(), kind=jnp.bfloat16):
    values = jax.random.normal(stream_key, dims, jnp.float32) * deviation
    if len(cuts) > 0:
        values = steps_of(stream_key, dims, cuts, -0.22, 0.18) * values
    return jnp.clip(values, min=-most, max=most).astype(kind)


def setup_inputs(seed: int = 0) -> dict:
    arg_keys = jax.random.split(jax.random.key(seed), 8)
    tokens = bell_draw(arg_keys[0], (TOKENS, D), 1.0, 6.0, ((0, 8),))
    route_logits = bell_draw(arg_keys[1], (TOKENS, TOP), 1.5, 6.0, (), jnp.float32)
    expert_ids_keys = jax.random.split(jax.random.fold_in(arg_keys[2], 1), TOKENS // TOKENS)
    expert_ids_turns = jax.random.permutation(jax.random.fold_in(arg_keys[2], 3), TOKENS // TOKENS)
    expert_ids = jax.vmap(lambda own, number: assign_block(jax.random.fold_in(arg_keys[2], 2), own, number, TOKENS, EXPERTS, TOP, CAP, 2))(expert_ids_keys, expert_ids_turns).reshape((TOKENS, TOP))
    block_live = place_ends((jax.random.randint(arg_keys[3], (EXPERTS, FF // BLK), 0, 4) < 3).astype(jnp.int32), jax.random.fold_in(arg_keys[3], 1), 0, 1)
    w_gate = bell_draw(arg_keys[4], (EXPERTS, D, FF), D ** -0.5, 0.09375, ((0, 4), (2, 8)))
    w_up = bell_draw(arg_keys[5], (EXPERTS, D, FF), D ** -0.5, 0.09375, ((0, 4), (2, 8)))
    w_down = bell_draw(arg_keys[6], (EXPERTS, FF, D), FF ** -0.5, 0.046875, ((0, 4), (1, 8)))
    return dict(tokens=tokens, route_logits=route_logits, expert_ids=expert_ids, block_live=block_live, w_gate=w_gate, w_up=w_up, w_down=w_down)


def routing(expert_ids, route_logits, expert, capacity):
    chosen = (expert_ids == expert).astype(jnp.int32)
    flat_hits = chosen.reshape(-1)
    before = (jnp.cumsum(flat_hits) - flat_hits).reshape(chosen.shape)
    slot_pair = jnp.where(chosen > 0, before, capacity).astype(jnp.int32)
    leading = jax.nn.sigmoid(route_logits[:, 0] - route_logits[:, 1])
    mix_gates = jnp.stack([leading, 1.0 - leading], axis=1)
    weight = jnp.sum(mix_gates * chosen.astype(jnp.float32), axis=1)
    slot_tok = jnp.min(slot_pair, axis=1)
    slot_index = lax.broadcasted_iota(jnp.int32, (capacity, expert_ids.shape[0]), 0)
    dispatch = ((slot_pair[None, :, 0] == slot_index) | (slot_pair[None, :, 1] == slot_index)).astype(jnp.bfloat16)
    return dispatch, slot_tok, weight


def reference(tokens, route_logits, expert_ids, block_live, w_gate, w_up, w_down):
    capacity = CAP
    result = jnp.zeros((TOKENS, D), jnp.float32)
    for expert in range(EXPERTS):
        dispatch, slot_tok, weight = routing(expert_ids, route_logits, expert, capacity)
        gathered = jnp.dot(dispatch, tokens, preferred_element_type=jnp.float32).astype(jnp.bfloat16)
        gate_val = jnp.dot(gathered, w_gate[expert], preferred_element_type=jnp.float32)
        up_val = jnp.dot(gathered, w_up[expert], preferred_element_type=jnp.float32)
        live = jnp.repeat(block_live[expert].astype(jnp.float32), BLK)
        hidden = (jax.nn.silu(gate_val) * up_val * live[None, :]).astype(jnp.bfloat16)
        expert_out = jnp.dot(hidden, w_down[expert], preferred_element_type=jnp.float32)
        picked = jnp.take(expert_out, jnp.minimum(slot_tok, capacity - 1), axis=0)
        result = result + weight[:, None] * picked
    return result.astype(jnp.bfloat16)
```

```python
import functools

import jax
import jax.numpy as jnp
from jax import lax
from jax.experimental import pallas as pl
from jax.experimental.pallas import tpu as pltpu
from jax.sharding import PartitionSpec as P

GROUPS = 4
TILE = 256
F32, BF16 = jnp.float32, jnp.bfloat16


def flipped(me, bit):
    return me + (1 - 2 * ((me // (1 << bit)) % 2)) * (1 << bit)


def bit_orders(bits):
    rest = list(range(1, bits))
    return ([0] + rest, [0] + rest[::-1])


def kernel(
    experts, neurons,
    ids_ref, logits_ref, live_ref, tok_hbm, wg_hbm, wu_hbm, wd_hbm,
    out_ref,
    wg, wu, wd, tb, xg, gate, up, hid, sb, rb, eb, fin, comb, combs, disps, sw, live,
    w_sem, t_sem, ag_s, ag_r, rs_s, rs_r, xr_s, xr_r, xa_s, xa_r,
):
    e = lax.axis_index("expert")
    me = lax.axis_index("neuron")
    bits = neurons.bit_length() - 1
    orders = bit_orders(bits)
    total, _ = ids_ref.shape
    rows, width = tok_hbm.shape
    capacity = total // 2
    cols = width // GROUPS
    part = cols // experts
    inner = wg.shape[1]
    tile = TILE if inner % TILE == 0 else inner
    out_tile = TILE if cols % TILE == 0 else cols

    tok_in = []
    for g in range(GROUPS):
        c = pltpu.make_async_copy(
            tok_hbm.at[:, pl.ds(g * cols, cols)], tb.at[g, pl.ds(0, rows)], t_sem.at[g])
        c.start()
        tok_in.append(c)
    up_in, down_in = [], []
    for g in range(GROUPS):
        k = pl.ds(g * cols, cols)
        pair = (pltpu.make_async_copy(wg_hbm.at[0, k], wg.at[k], w_sem.at[0, g]),
                pltpu.make_async_copy(wu_hbm.at[0, k], wu.at[k], w_sem.at[1, g]))
        for c in pair:
            c.start()
        up_in.append(pair)
    for g in range(GROUPS):
        c = pltpu.make_async_copy(wd_hbm.at[0, :, pl.ds(g * cols, cols)], wd.at[g], w_sem.at[2, g])
        c.start()
        down_in.append(c)

    barrier = pltpu.get_barrier_semaphore()
    for b in range(bits):
        pl.semaphore_signal(barrier, inc=1, device_id={"neuron": flipped(me, b)})
    for j in range(1, experts):
        pl.semaphore_signal(barrier, inc=1, device_id={"expert": (e + j) % experts})
    pl.semaphore_wait(barrier, bits + experts - 1)

    def gather_copy(g, step):
        count = rows << step
        bit = orders[g % 2][bits - 1 - step]
        return pltpu.make_async_remote_copy(
            src_ref=tb.at[g, pl.ds(0, count)], dst_ref=tb.at[g, pl.ds(count, count)],
            send_sem=ag_s.at[g, step], recv_sem=ag_r.at[g, step],
            device_id={"neuron": flipped(me, bit)})

    gathers = [[gather_copy(g, s) for s in range(bits)] for g in range(GROUPS)]
    for g in range(GROUPS):
        tok_in[g].wait()
        gathers[g][0].start()

    ids = ids_ref[...]
    logits = logits_ref[...]
    first, second = ids[:, 0:1] == e, ids[:, 1:2] == e
    chosen = jnp.where(first | second, 1.0, 0.0).astype(F32)
    leading = 1.0 / (1.0 + jnp.exp(logits[:, 1:2] - logits[:, 0:1]))
    weight = jnp.where(first, leading, 0.0) + jnp.where(second, 1.0 - leading, 0.0)
    tri = jnp.where(
        lax.broadcasted_iota(jnp.int32, (total, total), 1)
        < lax.broadcasted_iota(jnp.int32, (total, total), 0), 1.0, 0.0).astype(BF16)
    chosen_wide = jnp.broadcast_to(chosen, (total, capacity))
    slot = jnp.dot(tri, chosen_wide.astype(BF16), preferred_element_type=F32)
    lane = lax.broadcasted_iota(jnp.int32, (total, capacity), 1).astype(F32)
    one_hot = jnp.where(slot == lane, chosen_wide, 0.0)
    comb[...] = one_hot
    sw[...] = jnp.sum((one_hot * weight).T, axis=1, keepdims=True)
    for o in range(2):
        for p in range(neurons):
            owner = me
            for place, bit in enumerate(orders[o]):
                if (p >> (bits - 1 - place)) & 1:
                    owner = owner + (1 - 2 * ((me // (1 << bit)) % 2)) * (1 << bit)
            block = comb[pl.ds(pl.multiple_of(owner * rows, rows), rows), :]
            combs[o, pl.ds(p * rows, rows), :] = block.astype(BF16)
        disps[o] = combs[o].astype(F32).T.astype(BF16)

    blocks = live_ref.shape[1]
    number = lax.broadcasted_iota(jnp.int32, (8, inner), 1) // (inner // blocks)
    kept = jnp.zeros((8, inner), jnp.int32)
    for b in range(blocks):
        kept = jnp.where(number == b, live_ref[0, b], kept)
    live[...] = kept.astype(F32)

    def forward(g, step):
        gathers[g][step].wait_recv()
        if step + 1 < bits:
            gathers[g][step + 1].start()

    def gate_up(g):
        forward(g, bits - 1)
        xg[...] = jnp.dot(disps[g % 2], tb[g], preferred_element_type=F32).astype(BF16)
        for c in up_in[g]:
            c.wait()
        k = pl.ds(g * cols, cols)

        def body(i, carry):
            n = pl.ds(pl.multiple_of(i * tile, 128), tile) if inner > tile else pl.ds(0, tile)
            gv = jnp.dot(xg[...], wg[k, n], preferred_element_type=F32)
            uv = jnp.dot(xg[...], wu[k, n], preferred_element_type=F32)
            if g > 0:
                gv, uv = gv + gate[:, n], uv + up[:, n]
            if g < GROUPS - 1:
                gate[:, n] = gv
                up[:, n] = uv
            else:
                hid[:, n] = (gv / (1.0 + jnp.exp(-gv)) * uv * live[0:1, n]).astype(BF16)
            return carry

        lax.fori_loop(0, inner // tile, body, 0)

    for step in range(bits - 2):
        for g in range(GROUPS):
            forward(g, step)
    for lo in range(0, GROUPS, 2):
        for g in (lo, lo + 1):
            forward(g, bits - 2)
        for g in (lo, lo + 1):
            gate_up(g)

    def scatter_copy(g, step):
        half = total >> (step + 1)
        here = pl.ds(half, half)
        return pltpu.make_async_remote_copy(
            src_ref=sb.at[g, here], dst_ref=rb.at[g, here],
            send_sem=rs_s.at[g, step], recv_sem=rs_r.at[g, step],
            device_id={"neuron": flipped(me, orders[g % 2][step])})

    def peer_columns(g, who, base):
        return pl.ds(pl.multiple_of(base + who * part, 128), part)

    def combine_copy(g, j):
        who = (e + j) % experts
        return pltpu.make_async_remote_copy(
            src_ref=sb.at[g, pl.ds(0, rows), peer_columns(g, who, 0)], dst_ref=eb.at[g, j - 1],
            send_sem=xr_s.at[g, j - 1], recv_sem=xr_r.at[g, j - 1],
            device_id={"expert": who})

    def spread_copy(g, j):
        mine = fin.at[:, peer_columns(g, e, g * cols)]
        return pltpu.make_async_remote_copy(
            src_ref=mine, dst_ref=mine,
            send_sem=xa_s.at[g, j - 1], recv_sem=xa_r.at[g, j - 1],
            device_id={"expert": (e + j) % experts})

    scatters = [[scatter_copy(g, s) for s in range(bits)] for g in range(GROUPS)]
    combines = [[combine_copy(g, j) for j in range(1, experts)] for g in range(GROUPS)]
    spreads = [[spread_copy(g, j) for j in range(1, experts)] for g in range(GROUPS)]

    def down(g):
        down_in[g].wait()

        def body(i, carry):
            n = pl.ds(pl.multiple_of(i * out_tile, 128), out_tile)
            value = jnp.dot(hid[...], wd[g, :, n], preferred_element_type=F32)
            value = (value * sw[...]).astype(BF16)
            sb[g, :, n] = jnp.dot(combs[g % 2], value, preferred_element_type=F32).astype(BF16)
            return carry

        lax.fori_loop(0, cols // out_tile, body, 0)
        scatters[g][0].start()

    def reduce(g, step):
        half = total >> (step + 1)
        scatters[g][step].wait_recv()
        sb[g, pl.ds(0, half), :] = (
            sb[g, pl.ds(0, half), :].astype(F32) + rb[g, pl.ds(half, half), :].astype(F32)
        ).astype(BF16)
        if step + 1 < bits:
            scatters[g][step + 1].start()
        else:
            for c in combines[g]:
                c.start()

    def combine(g):
        value = sb[g, pl.ds(0, rows), peer_columns(g, e, 0)].astype(F32)
        for j, c in enumerate(combines[g]):
            c.wait_recv()
            value = value + eb[g, j].astype(F32)
        fin[:, peer_columns(g, e, g * cols)] = value.astype(BF16)
        for c in spreads[g]:
            c.start()

    for slot_no in range(GROUPS + bits + 1):
        if slot_no < GROUPS:
            down(slot_no)
        for g in range(GROUPS):
            stage = slot_no - g - 1
            if 0 <= stage < bits:
                reduce(g, stage)
            elif stage == bits:
                combine(g)

    for g in range(GROUPS):
        for c in spreads[g]:
            c.wait_recv()
    out_ref[...] = fin[...]
    for group in (gathers, scatters, combines, spreads):
        for copies in group:
            for c in copies:
                c.wait_send()


def per_device(experts, neurons, tokens, route_logits, expert_ids, block_live, w_gate, w_up, w_down):
    total = expert_ids.shape[0]
    rows, width = tokens.shape
    capacity = total // 2
    inner = w_gate.shape[2]
    cols = width // GROUPS
    bits = neurons.bit_length() - 1
    vmem = pl.BlockSpec(memory_space=pltpu.VMEM)
    hbm = pl.BlockSpec(memory_space=pl.ANY)
    dma = pltpu.SemaphoreType.DMA
    return pl.pallas_call(
        functools.partial(kernel, experts, neurons),
        out_shape=jax.ShapeDtypeStruct((rows, width), BF16),
        in_specs=[vmem, vmem, pl.BlockSpec(memory_space=pltpu.SMEM), hbm, hbm, hbm, hbm],
        out_specs=vmem,
        scratch_shapes=[
            pltpu.VMEM((width, inner), BF16),
            pltpu.VMEM((width, inner), BF16),
            pltpu.VMEM((GROUPS, inner, cols), BF16),
            pltpu.VMEM((GROUPS, total, cols), BF16),
            pltpu.VMEM((capacity, cols), BF16),
            pltpu.VMEM((capacity, inner), F32),
            pltpu.VMEM((capacity, inner), F32),
            pltpu.VMEM((capacity, inner), BF16),
            pltpu.VMEM((GROUPS, total, cols), BF16),
            pltpu.VMEM((GROUPS, total, cols), BF16),
            pltpu.VMEM((GROUPS, experts - 1, rows, cols // experts), BF16),
            pltpu.VMEM((rows, width), BF16),
            pltpu.VMEM((total, capacity), F32),
            pltpu.VMEM((2, total, capacity), BF16),
            pltpu.VMEM((2, capacity, total), BF16),
            pltpu.VMEM((capacity, 1), F32),
            pltpu.VMEM((8, inner), F32),
            dma((3, GROUPS)), dma((GROUPS,)),
            dma((GROUPS, bits)), dma((GROUPS, bits)),
            dma((GROUPS, bits)), dma((GROUPS, bits)),
            dma((GROUPS, experts - 1)), dma((GROUPS, experts - 1)),
            dma((GROUPS, experts - 1)), dma((GROUPS, experts - 1)),
        ],
        compiler_params=pltpu.CompilerParams(
            collective_id=0, has_side_effects=True, vmem_limit_bytes=67043328),
    )(expert_ids, route_logits, block_live, tokens, w_gate, w_up, w_down)


def solution(mesh):
    placed = (
        P("neuron", None),
        P(),
        P(),
        P("expert", "neuron"),
        P("expert", None, "neuron"),
        P("expert", None, "neuron"),
        P("expert", "neuron", None),
    )
    body = functools.partial(per_device, mesh.shape["expert"], mesh.shape["neuron"])
    return jax.shard_map(
        body, mesh=mesh, in_specs=placed, out_specs=P("neuron", None), check_vma=False
    )
```
